32 devices in a mesh: dp: 8 (over y, x, core), ctx: 4 (over z).
Axes of the slice: x: 2, y: 2, z: 4, core: 2. Of those that a mesh axis runs over, the one named last changes fastest.
Arguments:
- tokens: bfloat16 [16, 2048, 768], P('dp', 'ctx'), may hold values from -6 to 6
- cotangent: bfloat16 [16, 2048, 768], P('dp', 'ctx'), may hold values from -6 to 6
- proj_weights: float32 [1, 768, 2304], P(None, ('dp', 'ctx')), may hold values from -0.21875 to 0.21875
- out_weights: float32 [1, 768, 768], P(None, ('dp', 'ctx')), may hold values from -0.875 to 0.875
- router_weights: float32 [1, 768, 8], P(None, ('dp', 'ctx')), may hold values from -0.21875 to 0.21875
- norm_gains: float32 [1, 2, 768], replicated, may hold values from 0.5 to 1.5
- bias_table: float32 [1, 32, 12], replicated, may hold values from -4 to 4
- up_weights: float32 [1, 8, 768, 3072], P(None, 'dp', None, 'ctx'), may hold values from -0.21875 to 0.21875
- down_weights: float32 [1, 8, 3072, 768], P(None, 'dp', 'ctx'), may hold values from -0.109375 to 0.109375
- doc_lengths: int32 [16, 4], P('dp'), may hold values from 1 to 1536, 2048 in all within a row
- routes: int32 [16, 2048, 2], P('dp', 'ctx'), may hold values from 0 to 7, all different within a row
Outputs:
- result: bfloat16 [16, 2048, 768], P('dp', 'ctx')
- tokens_grad: bfloat16 [16, 2048, 768], P('dp', 'ctx')
- proj_grad: float32 [1, 768, 2304], P(None, ('dp', 'ctx'))
- out_grad: float32 [1, 768, 768], P(None, ('dp', 'ctx'))
- router_grad: float32 [1, 768, 8], P(None, ('dp', 'ctx'))
- gains_grad: float32 [1, 2, 768], replicated
- table_grad: float32 [1, 32, 12], replicated
- up_grad: float32 [1, 8, 768, 3072], P(None, 'dp', None, 'ctx')
- down_grad: float32 [1, 8, 3072, 768], P(None, 'dp', 'ctx')
The draws below stay inside these ranges and needn't reach their ends.
Inputs may be any that keep to these rules, and one draw needn't show every extreme that they name: `doc_lengths`: each row holds the lengths of its sequence's 4 documents; they sum to 2048 and the longest is 1536. `routes`: each token names 2 different experts, its first choice first.
All inputs are finite; a program needn't handle non-finite values.
Results may differ from the reference program's by a relative error of at most 0.02.
Values may be sent and summed in bfloat16 or wider, within the bound.
A program may use at most 384 MiB of HBM per device.

```python
import math
import jax
import jax.numpy as jnp
import numpy as np
from jax import lax

D = 768
HEADS = 12
HEAD_DIM = 64
FF = 3072
NB = 32
WIN = 1024
SEQ_LEN = 2048
NDOC = 4
TOP = 2
LAYERS = 1
EXPERTS = 8
NSEQ = 16
CAP = 160
DOC_MOST = 1536
N_CTX = 4


def shard_levels(key, extent, shards, low, top_value):
    level, own = 1.0, jax.random.fold_in(key, 6)
    for dim, parts in shards:
        heights = jnp.exp(jax.random.uniform(jax.random.fold_in(own, dim), (parts,), jnp.float32, low / len(shards), top_value / len(shards)))
        level = level * jnp.repeat(heights, extent[dim] // parts).reshape([-1 if axis == dim else 1 for axis in range(len(extent))])
    return level


def distinct(key, rows, amount, top, lift):
    ranking = jax.random.permutation(jax.random.fold_in(key, 1), amount)
    favour = ranking
    for power in range(3):
        favour = favour * favour // amount
    favour = favour * lift // amount
    tickets = jax.random.randint(jax.random.fold_in(key, 2), (rows, amount), 0, 4096) + favour
    fixed_rows = jax.random.permutation(jax.random.fold_in(key, 3), rows)[jnp.arange(amount) % rows]
    tickets = jnp.where(jnp.arange(rows)[:, None] == fixed_rows[None, :], 1 << 14, tickets)
    merit = tickets * amount + jnp.arange(amount)
    return lax.top_k(merit.astype(jnp.int32), top)[1].astype(jnp.int32)


def profile(amount, total, bound, lean):
    loads = [(1 << 20) // math.isqrt(grade ** lean) + 1 for grade in range(2, amount + 1)]
    spare, given = total - bound - (amount - 1), [1] * (amount - 1)
    while spare > 0:
        candidates = [i for i in range(amount - 1) if given[i] < bound]
        mass, budget = sum([loads[i] for i in candidates]), spare
        for i in candidates:
            extra = min(bound - given[i], max(1, budget * loads[i] // mass), spare)
            given[i] = given[i] + extra
            spare = spare - extra
    return np.array([bound] + given)


def ragged_sizes(stream_key, number_of, total, limit, slope):
    if number_of == 2:
        one = jax.random.randint(stream_key, (), max(1, total - limit), min(limit, total - 1) + 1)
        return jnp.stack([one, total - one])
    tallies = jnp.asarray(profile(number_of, total, limit, slope), jnp.int32)
    couples = (number_of - 1) // 2
    donor, sink = tallies[1:1 + 2 * couples:2], tallies[2:2 + 2 * couples:2]
    margin = jnp.minimum(donor - 1, limit - sink)
    shifted = jax.random.randint(jax.random.fold_in(stream_key, 1), (couples,), 0, 1 << 20) % (margin + 1)
    tallies = tallies.at[1:1 + 2 * couples:2].set(donor - shifted).at[2:2 + 2 * couples:2].set(sink + shifted)
    return tallies[jax.random.permutation(jax.random.fold_in(stream_key, 2), number_of)]


def gaussian(stream_key, extent, width, bound, cuts=(), kind=jnp.bfloat16):
    factor_of = shard_levels(stream_key, extent, cuts, -0.22, 0.18) if cuts else 1.0
    entries = jax.random.normal(stream_key, extent, jnp.float32) * width * factor_of
    return jnp.minimum(jnp.maximum(entries, -bound), bound).astype(kind)


def setup_inputs(seed: int = 0) -> dict:
    key_of = jax.random.split(jax.random.key(seed), 12)
    tokens = gaussian(key_of[0], (NSEQ, SEQ_LEN, D), 1.0, 6.0, ((0, 8), (1, 4)))
    cotangent = gaussian(key_of[1], (NSEQ, SEQ_LEN, D), 1.0, 6.0, ((0, 8), (1, 4)))
    proj_weights = gaussian(key_of[2], (LAYERS, D, 3 * D), D ** -0.5, 0.21875, ((1, 32),), jnp.float32)
    out_weights = gaussian(key_of[3], (LAYERS, D, D), (D // 16) ** -0.5, 0.875, ((1, 32),), jnp.float32)
    router_weights = gaussian(key_of[4], (LAYERS, D, EXPERTS), D ** -0.5, 0.21875, ((1, 32),), jnp.float32)
    norm_gains = jnp.clip(1.0 + 0.1 * jax.random.normal(key_of[5], (LAYERS, 2, D), jnp.float32), 0.5, 1.5)
    bias_table = gaussian(key_of[6], (LAYERS, NB, HEADS), 1.0, 4.0, (), jnp.float32)
    up_weights = gaussian(key_of[7], (LAYERS, EXPERTS, D, FF), D ** -0.5, 0.21875, ((1, 8), (3, 4)), jnp.float32)
    down_weights = gaussian(key_of[8], (LAYERS, EXPERTS, FF, D), FF ** -0.5, 0.109375, ((1, 8), (2, 4)), jnp.float32)
    doc_lengths = jax.vmap(lambda own: ragged_sizes(own, NDOC, SEQ_LEN, DOC_MOST, 2))(jax.random.split(key_of[9], NSEQ)).reshape((NSEQ, NDOC)).astype(jnp.int32)
    routes = distinct(key_of[10], NSEQ * SEQ_LEN, EXPERTS, TOP, 2048).reshape((NSEQ, SEQ_LEN, TOP))
    return dict(tokens=tokens, cotangent=cotangent, proj_weights=proj_weights, out_weights=out_weights, router_weights=router_weights, norm_gains=norm_gains, bias_table=bias_table, up_weights=up_weights, down_weights=down_weights, doc_lengths=doc_lengths, routes=routes)


EPS = 1e-06
NEG = -1e+30
HIGH = lax.Precision.HIGHEST
BUCKET_EDGES = [16, 21, 27, 35, 45, 58, 76, 98, 128, 166, 215, 279, 362, 470, 609, 790]

@jax.custom_vjp
def low(v):
    return lax.optimization_barrier(v.astype(jnp.bfloat16)).astype(jnp.float32)

@jax.custom_vjp
def low_back(v):
    return v

def low_keep(v):
    return (low(v), None)

def low_pass(kept, grad):
    return (grad,)

def back_keep(v):
    return (v, None)

def back_low(kept, grad):
    return (low(grad),)
low.defvjp(low_keep, low_pass)
low_back.defvjp(back_keep, back_low)

def rms_norm(operand, gain_vec):
    return operand * lax.rsqrt(lax.optimization_barrier(jnp.mean(operand * operand, axis=-1, keepdims=True)) + EPS) * gain_vec

def bucket_index(distance):
    edge_values = jnp.array(BUCKET_EDGES, dtype=jnp.int32)
    passed = lax.optimization_barrier(jnp.sum((distance[..., None] >= edge_values).astype(jnp.int32), axis=-1)).astype(jnp.int32)
    return jnp.where(distance < 16, distance, 15 + passed).astype(jnp.int32)

def doc_of(positions, lengths):
    bounds = jnp.cumsum(lengths).astype(jnp.int32)[:-1]
    return lax.optimization_barrier(jnp.sum((positions[:, None] >= bounds[None, :]).astype(jnp.int32), axis=-1)).astype(jnp.int32)

def attend_sequence(query_rows, key_rows, value_rows, doc_ids, table):
    block_rows = min(512, SEQ_LEN)
    block_count = SEQ_LEN // block_rows
    key_pos = jnp.arange(SEQ_LEN, dtype=jnp.int32)

    def one_block(start_row):
        queries = lax.dynamic_slice_in_dim(query_rows, start_row, block_rows, 0)
        query_docs = lax.dynamic_slice_in_dim(doc_ids, start_row, block_rows, 0)
        query_pos = start_row + jnp.arange(block_rows, dtype=jnp.int32)
        distance = (query_pos[:, None] - key_pos[None, :]).astype(jnp.int32)
        allowed = (distance >= 0) & (distance < WIN) & (query_docs[:, None] == doc_ids[None, :])
        rel_bias = jnp.take(table, jnp.clip(bucket_index(distance), 0, NB - 1), axis=0)
        raw_scores = jnp.einsum('qhd,khd->hqk', queries, key_rows, precision=HIGH) * HEAD_DIM ** (-0.5) + jnp.transpose(rel_bias, (2, 0, 1))
        masked = jnp.where(allowed[None], low_back(raw_scores), NEG)
        attn_probs = low(jax.nn.softmax(masked, axis=-1))
        return jnp.einsum('hqk,khd->qhd', attn_probs, value_rows, precision=HIGH)
    starts = jnp.arange(block_count, dtype=jnp.int32) * block_rows
    blocks = lax.map(jax.checkpoint(one_block), starts)
    return blocks.reshape(SEQ_LEN, HEADS * HEAD_DIM)

def expert_apply(packed):
    rows_in, up_one, down_one = packed
    pre_act = low_back(jnp.dot(rows_in, up_one, precision=HIGH))
    hidden = low(jax.nn.gelu(pre_act, approximate=True))
    return low(low_back(jnp.dot(hidden, down_one, precision=HIGH)))

def layer_forward(resid, proj, out_mat, router, gains_now, table, up_mat, down_mat, doc_ids, routes):
    normed = low(rms_norm(resid, gains_now[0]))
    mixed_qkv = low(low_back(jnp.einsum('std,de->ste', normed, low(proj), precision=HIGH)))
    head_shape = (NSEQ, SEQ_LEN, HEADS, HEAD_DIM)
    queries = mixed_qkv[..., :D].reshape(head_shape)
    key_rows = mixed_qkv[..., D:2 * D].reshape(head_shape)
    value_rows = mixed_qkv[..., 2 * D:].reshape(head_shape)

    def attend_one(packed):
        return attend_sequence(packed[0], packed[1], packed[2], packed[3], table)
    attended = lax.map(attend_one, (queries, key_rows, value_rows, doc_ids))
    attn_low = low(low_back(attended))
    middle = resid + low_back(jnp.einsum('std,de->ste', attn_low, low(out_mat), precision=HIGH))
    two_low = low(rms_norm(middle, gains_now[1]))
    logits = low_back(jnp.einsum('std,de->ste', two_low, low(router), precision=HIGH))
    soft_probs = jax.nn.softmax(logits, axis=-1)
    chosen = jnp.take_along_axis(soft_probs, routes, axis=-1)
    gate_vals = chosen / lax.optimization_barrier(jnp.sum(chosen, axis=-1, keepdims=True))
    groups = NSEQ * N_CTX
    tok_rows = SEQ_LEN // N_CTX
    grouped = two_low.reshape(groups, tok_rows, D)
    route_groups = routes.reshape(groups, tok_rows, TOP)
    gate_groups = gate_vals.reshape(groups, tok_rows, TOP)
    order_ids = jnp.transpose(route_groups, (0, 2, 1)).reshape(groups, TOP * tok_rows)
    order_hot = (order_ids[..., None] == jnp.arange(EXPERTS, dtype=jnp.int32)).astype(jnp.int32)
    running = jnp.cumsum(order_hot, axis=1).astype(jnp.int32)
    slot_pos = (lax.optimization_barrier(jnp.sum(running * order_hot, axis=-1)).astype(jnp.int32) - 1).reshape(groups, TOP, tok_rows)
    group_ids = jnp.arange(groups, dtype=jnp.int32)[:, None]
    filled = jnp.zeros((groups, EXPERTS * CAP + 1, D), jnp.float32)
    slot_list = []
    for rank_idx in range(TOP):
        position = slot_pos[:, rank_idx]
        slot_now = jnp.where(position < CAP, route_groups[:, :, rank_idx] * CAP + position, EXPERTS * CAP).astype(jnp.int32)
        slot_list.append(slot_now)
        filled = filled.at[group_ids, slot_now].add(grouped)
    expert_in = low_back(filled[:, :EXPERTS * CAP].reshape(groups, EXPERTS, CAP, D))
    by_expert = jnp.transpose(expert_in, (1, 0, 2, 3)).reshape(EXPERTS, groups * CAP, D)
    expert_out = lax.map(jax.checkpoint(expert_apply), (by_expert, low(up_mat), low(down_mat)))
    back_rows = jnp.transpose(expert_out.reshape(EXPERTS, groups, CAP, D), (1, 0, 2, 3)).reshape(groups, EXPERTS * CAP, D)
    back_rows = jnp.concatenate([back_rows, jnp.zeros((groups, 1, D), jnp.float32)], axis=1)
    combined = jnp.zeros((groups, tok_rows, D), jnp.float32)
    for rank_idx in range(TOP):
        combined = combined + gate_groups[:, :, rank_idx, None] * back_rows[group_ids, slot_list[rank_idx]]
    return middle + combined.reshape(NSEQ, SEQ_LEN, D)

def reference(tokens, cotangent, proj_weights, out_weights, router_weights, norm_gains, bias_table, up_weights, down_weights, doc_lengths, routes):
    seq_pos = jnp.arange(SEQ_LEN, dtype=jnp.int32)
    doc_ids = jax.vmap(lambda lens_row: doc_of(seq_pos, lens_row))(doc_lengths)

    def forward(resid, proj, out_mat, router, gains, table, up_mat, down_mat):
        for layer_idx in range(LAYERS):
            resid = layer_forward(resid, proj[layer_idx], out_mat[layer_idx], router[layer_idx], gains[layer_idx], table[layer_idx], up_mat[layer_idx], down_mat[layer_idx], doc_ids, routes)
        return resid
    output, pullback = jax.vjp(forward, tokens.astype(jnp.float32), proj_weights, out_weights, router_weights, norm_gains, bias_table, up_weights, down_weights)
    grads = pullback(cotangent.astype(jnp.float32))
    return (output.astype(jnp.bfloat16), grads[0].astype(jnp.bfloat16), grads[1], grads[2], grads[3], grads[4], grads[5], grads[6], grads[7])
```

```python
from functools import partial

import jax
import jax.numpy as jnp
from jax import lax
from jax.experimental import pallas as pl
from jax.experimental.pallas import tpu as pltpu
from jax.sharding import PartitionSpec as P

HEADS=12; HEAD_DIM=64; NB=32; WIN=1024; TOP=2
NEG=-1e30
BUCKET_EDGES = [16, 21, 27, 35, 45, 58, 76, 98, 128, 166, 215, 279, 362, 470, 609, 790]
QB=256; CB=256; SPAN=WIN+QB; GROWS=SPAN+128; GSEG=GROWS//128

NT=(((1,),(1,)),((),()))
NN=(((1,),(0,)),((),()))
def dot(a,b,dims): return lax.dot_general(a,b,dims,preferred_element_type=jnp.float32)

def bucket_index(distance):
    edge_values = jnp.array(BUCKET_EDGES, dtype=jnp.int32)
    passed = jnp.sum((distance[..., None] >= edge_values).astype(jnp.int32), axis=-1)
    return jnp.where(distance < 16, distance, 15 + passed)

def bias_line(table):
    n = GROWS + 128
    d = jnp.arange(n, dtype=jnp.int32) - 256
    hot = (jnp.clip(bucket_index(d),0,NB-1)[:,None]==jnp.arange(NB)).astype(jnp.float32)
    line = jnp.einsum("nb,bh->hn", hot, table, precision=lax.Precision.HIGHEST)
    line = jnp.where((d>=0)&(d<WIN), line, NEG)
    return line.reshape(HEADS//2,2,n)

def spread_bias(line_ref, g_ref):
    for hh in range(2):
        for a in range(GSEG):
            start = (GSEG-1-a)*128
            seg = line_ref[0, hh:hh+1, start:start+256]
            x = jnp.broadcast_to(seg,(128,256))
            x = pltpu.roll(x,0,1,stride=1,stride_axis=0)
            g_ref[hh, a*128:(a+1)*128,:] = x[:,128:256]

def bias_chunk(g_ref, hh, r):
    o = pl.multiple_of(r*CB,CB) if not isinstance(r,int) else r*CB
    return jnp.concatenate([g_ref[hh, pl.ds(o+128,CB),:], g_ref[hh, pl.ds(o,CB),:]],axis=1)

def rows8(x, op):
    return op(x.reshape(x.shape[0]//8,8,x.shape[1]),axis=0)

def fwd_kernel(c0, line_ref, q_ref, k_ref, v_ref, qf_ref, kf_ref, o_ref, lse_ref, g_ref, kh_ref, qh_ref, vt_ref, s_ref, ot_ref):
    T=q_ref.shape[1]
    @pl.when(pl.program_id(1)==0)
    def _(): spread_bias(line_ref,g_ref)
    lane = lax.broadcasted_iota(jnp.int32,(1,128),1)
    vt_ref[...] = v_ref[0].T
    for hh in range(2):
        mine = (lane//64)==hh
        kh_ref[...] = jnp.where(mine,k_ref[0],kf_ref[0])
        qh_ref[...] = jnp.where(mine,q_ref[0],qf_ref[0])
        for b in range(T//QB):
            qb = qh_ref[b*QB:(b+1)*QB,:]
            mx=None
            for r in range(SPAN//CB):
                base=b*QB+c0+r*CB
                s=dot(kh_ref[base:base+CB,:],qb,NT)+bias_chunk(g_ref,hh,r)
                s_ref[r]=s
                m8=rows8(s,jnp.max)
                mx=m8 if mx is None else jnp.maximum(mx,m8)
            m=jnp.max(mx,axis=0,keepdims=True)
            tot=None; acc=None
            for r in range(SPAN//CB):
                base=b*QB+c0+r*CB
                p=jnp.exp(s_ref[r]-m)
                t8=rows8(p,jnp.sum)
                tot=t8 if tot is None else tot+t8
                d=dot(vt_ref[64*hh:64*hh+64,base:base+CB],p.astype(jnp.bfloat16),NN)
                acc=d if acc is None else acc+d
            l=jnp.sum(tot,axis=0,keepdims=True)
            ot_ref[64*hh:64*hh+64,b*QB:(b+1)*QB]=acc*(1.0/l)
            lse_ref[0,0,hh:hh+1,b*QB:(b+1)*QB]=m+jnp.log(l)
    o_ref[0]=ot_ref[...].T.astype(jnp.bfloat16)

def attn_forward(line,q,kv,qf,kf,c0):
    B,T,D=q.shape; K=kv.shape[1]; PR=D//128
    return pl.pallas_call(
        partial(fwd_kernel,c0),
        grid=(PR,B),
        in_specs=[pl.BlockSpec((1,2,line.shape[2]),lambda p,m:(p,0,0)),
                  pl.BlockSpec((1,T,128),lambda p,m:(m,0,p)),
                  pl.BlockSpec((1,K,128),lambda p,m:(m,0,p)),
                  pl.BlockSpec((1,K,128),lambda p,m:(m,0,PR+p)),
                  pl.BlockSpec((1,T,128),lambda p,m:(m,0,0)),
                  pl.BlockSpec((1,K,128),lambda p,m:(m,0,0))],
        out_specs=[pl.BlockSpec((1,T,128),lambda p,m:(m,0,p)),
                   pl.BlockSpec((1,1,2,T),lambda p,m:(m,p,0,0))],
        out_shape=[jax.ShapeDtypeStruct((B,T,D),jnp.bfloat16),jax.ShapeDtypeStruct((B,PR,2,T),jnp.float32)],
        scratch_shapes=[pltpu.VMEM((2,GROWS,128),jnp.float32),pltpu.VMEM((K,128),jnp.bfloat16),pltpu.VMEM((T,128),jnp.bfloat16),
                        pltpu.VMEM((128,K),jnp.bfloat16),pltpu.VMEM((SPAN//CB,CB,QB),jnp.float32),pltpu.VMEM((128,T),jnp.float32)],
        cost_estimate=pl.CostEstimate(flops=4*B*D*T*SPAN,bytes_accessed=2*B*D*(2*T+2*K),transcendentals=B*HEADS*T*SPAN),
    )(line,q,kv,kv,qf,kf)

def bwd_kernel(c0, line_ref, q_ref, k_ref, v_ref, g_ref_in, qf_ref, kf_ref, lse_ref, dl_ref, dq_ref, dk_ref, dv_ref, tg_ref,
               g_ref, kh_ref, qh_ref, qz_ref, dz_ref, kt_ref, dk_acc, dv_acc, dqt_acc, t_acc):
    T=q_ref.shape[1]
    last=pl.num_programs(1)-1
    @pl.when(pl.program_id(1)==0)
    def _():
        spread_bias(line_ref,g_ref)
        t_acc[...]=jnp.zeros_like(t_acc)
    lane = lax.broadcasted_iota(jnp.int32,(1,128),1)
    kt_ref[...] = k_ref[0].T
    dk_acc[...]=jnp.zeros_like(dk_acc)
    dv_acc[...]=jnp.zeros_like(dv_acc)
    for hh in range(2):
        mine = (lane//64)==hh
        kh_ref[hh] = jnp.where(mine,k_ref[0],kf_ref[0])
        qh_ref[hh] = jnp.where(mine,q_ref[0],qf_ref[0])
        qz_ref[hh] = jnp.where(mine,q_ref[0],jnp.zeros_like(q_ref[0]))
        dz_ref[hh] = jnp.where(mine,g_ref_in[0],jnp.zeros_like(q_ref[0]))
    dqt_acc[...]=jnp.zeros_like(dqt_acc)
    nb=T//QB
    def step(r,carry):
        for b in range(nb):
            for hh in range(2):
                base=pl.multiple_of(b*QB+c0+r*CB,128)
                keys=pl.ds(base,CB)
                rows=slice(b*QB,(b+1)*QB)
                s=dot(kh_ref[hh,keys,:],qh_ref[hh,rows,:],NT)+bias_chunk(g_ref,hh,r)
                p=jnp.exp(s-lse_ref[0,0,hh:hh+1,rows])
                dp=dot(v_ref[0,keys,:],dz_ref[hh,rows,:],NT)
                ds=p*(dp-dl_ref[0,0,hh:hh+1,rows])
                dsb=ds.astype(jnp.bfloat16)
                dv_acc[keys,:]+=dot(p.astype(jnp.bfloat16),dz_ref[hh,rows,:],NN)
                dk_acc[keys,:]+=dot(dsb,qz_ref[hh,rows,:],NN)
                dqt_acc[64*hh:64*hh+64,rows]+=dot(kt_ref[64*hh:64*hh+64,keys],dsb,NN)
                o=pl.multiple_of(r*CB,CB)
                t_acc[hh,pl.ds(o+128,CB),:]+=ds[:,:128]
                t_acc[hh,pl.ds(o,CB),:]+=ds[:,128:]
        return carry
    lax.fori_loop(0,SPAN//CB,step,0)
    dk_ref[0]=dk_acc[...].astype(jnp.bfloat16)
    dv_ref[0]=dv_acc[...].astype(jnp.bfloat16)
    dq_ref[0]=(dqt_acc[...].T*(HEAD_DIM**-0.5)).astype(jnp.bfloat16)
    @pl.when(pl.program_id(1)==last)
    def _():
        flip=(lax.broadcasted_iota(jnp.int32,(128,128),0)+lax.broadcasted_iota(jnp.int32,(128,128),1)==127).astype(jnp.float32)
        for hh in range(2):
            for a in range(GSEG):
                blk=lax.dot_general(flip,t_acc[hh,a*128:(a+1)*128,:],NN,precision=lax.Precision.HIGHEST,preferred_element_type=jnp.float32)
                x=jnp.concatenate([blk,jnp.zeros_like(blk)],axis=1)
                x=pltpu.roll(x,0,1,stride=1,stride_axis=0)
                tg_ref[0,hh,a:a+1,:]=jnp.sum(x,axis=0,keepdims=True)

def attn_backward(line,q,kv,do,qf,kf,lse,dl,c0):
    B,T,D=q.shape; K=kv.shape[1]; PR=D//128
    return pl.pallas_call(
        partial(bwd_kernel,c0),
        grid=(PR,B),
        in_specs=[pl.BlockSpec((1,2,line.shape[2]),lambda p,m:(p,0,0)),
                  pl.BlockSpec((1,T,128),lambda p,m:(m,0,p)),
                  pl.BlockSpec((1,K,128),lambda p,m:(m,0,p)),
                  pl.BlockSpec((1,K,128),lambda p,m:(m,0,PR+p)),
                  pl.BlockSpec((1,T,128),lambda p,m:(m,0,p)),
                  pl.BlockSpec((1,T,128),lambda p,m:(m,0,0)),
                  pl.BlockSpec((1,K,128),lambda p,m:(m,0,0)),
                  pl.BlockSpec((1,1,2,T),lambda p,m:(m,p,0,0)),
                  pl.BlockSpec((1,1,2,T),lambda p,m:(m,p,0,0))],
        out_specs=[pl.BlockSpec((1,T,128),lambda p,m:(m,0,p)),
                   pl.BlockSpec((1,K,128),lambda p,m:(m,0,p)),
                   pl.BlockSpec((1,K,128),lambda p,m:(m,0,p)),
                   pl.BlockSpec((1,2,GSEG,256),lambda p,m:(p,0,0,0))],
        out_shape=[jax.ShapeDtypeStruct((B,T,D),jnp.bfloat16),jax.ShapeDtypeStruct((B,K,D),jnp.bfloat16),
                   jax.ShapeDtypeStruct((B,K,D),jnp.bfloat16),jax.ShapeDtypeStruct((PR,2,GSEG,256),jnp.float32)],
        scratch_shapes=[pltpu.VMEM((2,GROWS,128),jnp.float32),pltpu.VMEM((2,K,128),jnp.bfloat16),pltpu.VMEM((2,T,128),jnp.bfloat16),
                        pltpu.VMEM((2,T,128),jnp.bfloat16),pltpu.VMEM((2,T,128),jnp.bfloat16),pltpu.VMEM((128,K),jnp.bfloat16),
                        pltpu.VMEM((K,128),jnp.float32),pltpu.VMEM((K,128),jnp.float32),pltpu.VMEM((128,T),jnp.float32),
                        pltpu.VMEM((2,GROWS,128),jnp.float32)],
        cost_estimate=pl.CostEstimate(flops=10*B*D*T*SPAN,bytes_accessed=2*B*D*(2*T+2*K)*2,transcendentals=B*HEADS*T*SPAN),
    )(line,q,kv,kv,do,qf,kf,lse,dl)

def table_from_diagonals(diag):
    d = WIN+128-128*jnp.arange(GSEG)[:,None]+(jnp.arange(256)[None,:]-127)
    hot=(jnp.clip(bucket_index(d),0,NB-1)[...,None]==jnp.arange(NB)).astype(jnp.float32)
    hot=hot*((d>=0)&(d<WIN)).astype(jnp.float32)[...,None]
    h=diag.reshape(HEADS,GSEG*256)
    return jnp.einsum("hn,nb->bh",h,hot.reshape(GSEG*256,NB),precision=lax.Precision.HIGHEST)

def features(qdoc,kdoc,kvalid):
    lane=jnp.arange(128)%64
    qf=(qdoc[...,None]==lane).astype(jnp.bfloat16)
    bad=(kdoc[...,None]!=lane)|~kvalid[...,None]
    kf=jnp.where(bad&(lane<8),NEG,0.0).astype(jnp.bfloat16)
    return qf,kf


GELU_C = 0.7978845608028654
GELU_A = 0.044715


def row_step(rows):
    for size in (256, 128, 64, 32, 16):
        if rows % size == 0:
            return size
    return rows


def expert_kernel(with_prior, xg_ref, up_ref, dn_ref, *refs):
    if with_prior:
        pu_ref, pd_ref, ret_ref, ug_ref, dg_ref, acc, xt, gt, hb, zb = refs
    else:
        ret_ref, ug_ref, dg_ref, acc, xt, gt, hb, zb = refs
    R = xg_ref.shape[0]
    D = xg_ref.shape[1] // 2
    RB = row_step(R)

    @pl.when(pl.program_id(0) == 0)
    def _():
        xt[...] = xg_ref[:, :D].T
        gt[...] = xg_ref[:, D:].T
        acc[...] = jnp.zeros_like(acc)

    up = up_ref[...]
    dn = dn_ref[...]

    def block(i, carry):
        rs = pl.ds(pl.multiple_of(i * RB, RB), RB)
        z = dot(xg_ref[rs, :D], up, NN)
        dh = dot(xg_ref[rs, D:], dn, NT)
        zz = z * z
        t = jnp.tanh(z * (GELU_C + (GELU_C * GELU_A) * zz))
        half = 0.5 + 0.5 * t
        h = (z * half).astype(jnp.bfloat16)
        slope = half + z * (0.5 - 0.5 * t * t) * (GELU_C + (3.0 * GELU_C * GELU_A) * zz)
        dz = (dh * slope).astype(jnp.bfloat16)
        hb[rs, :] = h
        zb[rs, :] = dz
        acc[rs, :D] += dot(h, dn, NN)
        acc[rs, D:] += dot(dz, up, NT)
        return carry

    lax.fori_loop(0, R // RB, block, 0)
    ug = dot(xt[...], zb[...], NN)
    dg = dot(gt[...], hb[...], NN)
    if with_prior:
        ug += pu_ref[...]
        dg += pd_ref[...]
    ug_ref[...] = ug.astype(ug_ref.dtype)
    dg_ref[...] = dg.astype(dg_ref.dtype)

    @pl.when(pl.program_id(0) == pl.num_programs(0) - 1)
    def _():
        ret_ref[...] = acc[...].astype(jnp.bfloat16)


def expert_step(xg, up, dn, prior, last):
    R, D2 = xg.shape
    D, F = up.shape
    FC = 512
    wide = pl.BlockSpec((D, FC), lambda f: (0, f))
    tall = pl.BlockSpec((FC, D), lambda f: (f, 0))
    whole = pl.BlockSpec((R, D2), lambda f: (0, 0))
    grad_type = jnp.bfloat16 if last else jnp.float32
    return pl.pallas_call(
        partial(expert_kernel, prior is not None),
        grid=(F // FC,),
        in_specs=[whole, wide, tall] + ([wide, wide] if prior is not None else []),
        out_specs=[whole, wide, wide],
        out_shape=[
            jax.ShapeDtypeStruct((R, D2), jnp.bfloat16),
            jax.ShapeDtypeStruct((D, F), grad_type),
            jax.ShapeDtypeStruct((D, F), grad_type),
        ],
        scratch_shapes=[
            pltpu.VMEM((R, D2), jnp.float32),
            pltpu.VMEM((D, R), jnp.bfloat16),
            pltpu.VMEM((D, R), jnp.bfloat16),
            pltpu.VMEM((R, FC), jnp.bfloat16),
            pltpu.VMEM((R, FC), jnp.bfloat16),
        ],
        cost_estimate=pl.CostEstimate(
            flops=12 * R * D * F, bytes_accessed=8 * D * F + 8 * R * D, transcendentals=R * F
        ),
    )(xg, up, dn, *(prior if prior is not None else ()))


EPS = 1e-06


def passed_along(block, axis, distance):
    devices = range(lax.axis_size(axis))
    route = [(i - distance, i) for i in devices if i - distance in devices]
    return lax.ppermute(block, axis, route)


def rms_norm(operand, gain_vec):
    return operand * lax.rsqrt(jnp.mean(operand * operand, axis=-1, keepdims=True) + EPS) * gain_vec


def doc_of(positions, lengths):
    bounds = jnp.cumsum(lengths)[:-1]
    return jnp.sum((positions[:, None] >= bounds[None, :]).astype(jnp.int32), axis=-1)


def gate_values(logits, route_picks):
    soft_probs = jax.nn.softmax(logits, axis=-1)
    chosen = jnp.sum(soft_probs[:, None, :] * route_picks, axis=-1)
    return chosen / jnp.sum(chosen, axis=-1, keepdims=True)


def exchange(payload, ranks):
    shape = payload.shape
    blocks = payload.reshape(ranks, shape[0] // ranks, shape[1])
    return lax.all_to_all(blocks, "dp", split_axis=0, concat_axis=0, tiled=True).reshape(shape)


def mm(a, b):
    return jnp.dot(a, b, preferred_element_type=jnp.float32)


def on_device(
    tokens,
    cotangent,
    proj_weights,
    out_weights,
    router_weights,
    norm_gains,
    bias_table,
    up_weights,
    down_weights,
    doc_lengths,
    routes,
):
    B, T, D = tokens.shape
    low = jnp.bfloat16
    ranks = lax.axis_size("dp")
    experts = ranks * up_weights.shape[1]
    capacity = max(2, 5 * TOP * T // (4 * experts))
    slots = experts * capacity
    hops = (WIN + T - 2) // T
    K = (hops + 1) * T
    c0 = K - T - WIN
    base_pos = lax.axis_index("ctx") * T

    x_own = tokens
    pieces = [x_own]
    moving = x_own
    for _ in range(hops):
        moving = passed_along(moving, "ctx", 1)
        pieces.append(moving)
    x_all = jnp.concatenate(pieces[::-1], axis=1)

    router_pad = jnp.pad(router_weights[0], ((0, 0), (0, 128 - experts)))
    dense = jnp.concatenate([proj_weights[0], out_weights[0], router_pad], axis=1).astype(low)
    dense_full = lax.all_gather(dense, ("dp", "ctx"), axis=0, tiled=True)
    up_full = lax.all_gather(up_weights[0, 0].astype(low), "ctx", axis=1, tiled=True)
    dn_full = lax.all_gather(down_weights[0, 0].astype(low), "ctx", axis=0, tiled=True)
    w_q, w_k, w_v = (dense_full[:, i * D : (i + 1) * D] for i in range(3))
    w_kv = dense_full[:, D : 3 * D]
    w_out = dense_full[:, 3 * D : 4 * D]
    w_router = dense_full[:, 4 * D : 4 * D + experts]
    gains = norm_gains[0]

    line = bias_line(bias_table[0])
    rows = jnp.arange(T, dtype=jnp.int32)
    key_pos = base_pos - (K - T) + jnp.arange(K, dtype=jnp.int32)
    key_doc = jnp.stack([doc_of(key_pos, doc_lengths[m]) for m in range(B)])
    key_ok = jnp.broadcast_to(key_pos >= 0, (B, K))
    qf, kf = features(key_doc[:, K - T :], key_doc, key_ok)

    normed = rms_norm(x_all.astype(jnp.float32), gains[0]).astype(low)
    kv = mm(normed.reshape(B * K, D), w_kv).astype(low).reshape(B, K, 2 * D)
    normed_own = normed[:, K - T :]
    q = (mm(normed_own.reshape(B * T, D), w_q).astype(low) * low(HEAD_DIM**-0.5)).reshape(B, T, D)

    attn, lse = attn_forward(line, q, kv, qf, kf, c0)

    expert_ids = jnp.arange(experts, dtype=jnp.int32)
    slot_range = jnp.arange(slots, dtype=jnp.int32)
    kept = []
    for m in range(B):
        route_now = routes[m]
        picks = (route_now[:, :, None] == expert_ids).astype(jnp.float32)
        order_hot = (jnp.transpose(route_now).reshape(-1)[:, None] == expert_ids[None, :]).astype(
            jnp.int32
        )
        running = jnp.cumsum(order_hot, axis=0)
        slot_pos = (jnp.sum(running * order_hot, axis=-1) - 1).reshape(TOP, T)
        slot_ids = jnp.transpose(route_now) * capacity + slot_pos
        slot_ids = jnp.where(slot_pos < capacity, slot_ids, slots)
        hot = slot_ids[:, None, :] == slot_range[None, :, None]
        table = (hot[0] | hot[1]).astype(low)

        resid = tokens[m].astype(jnp.float32)
        d_out = cotangent[m]
        middle = resid + mm(attn[m], w_out)
        two_low = rms_norm(middle, gains[1]).astype(low)
        logits = mm(two_low, w_router)
        gates = gate_values(logits, picks)
        slot_gate = jnp.sum(
            jnp.where(hot[0], gates[None, :, 0], 0.0) + jnp.where(hot[1], gates[None, :, 1], 0.0),
            axis=1,
        )
        sent = mm(table, jnp.concatenate([two_low, d_out], axis=1))
        d_rows = sent[:, D:].astype(low)
        payload = jnp.concatenate(
            [sent[:, :D].astype(low), (sent[:, D:] * slot_gate[:, None]).astype(low)], axis=1
        )
        received = exchange(payload, ranks)
        kept.append((picks, hot, table, middle, two_low, logits, slot_gate, d_rows, received))

    prior = None
    returned = []
    for m in range(B):
        last = m == B - 1
        back, up_part, dn_part = expert_step(kept[m][-1], up_full, dn_full, prior, last)
        prior = (up_part, dn_part)
        returned.append(exchange(back, ranks))
    up_part, dn_part = prior
    up_grad = lax.psum_scatter(up_part, "ctx", scatter_dimension=1, tiled=True)
    dn_grad = lax.psum_scatter(dn_part, "ctx", scatter_dimension=1, tiled=True)

    outputs = []
    mids = []
    d_branches = []
    d_attns = []
    router_grad = 0.0
    gain_two = 0.0
    for m in range(B):
        picks, hot, table, middle, two_low, logits, slot_gate, d_rows, _ = kept[m]
        back = returned[m]
        d_resid = cotangent[m].astype(jnp.float32)
        slot_dgate = jnp.sum(d_rows.astype(jnp.float32) * back[:, :D].astype(jnp.float32), axis=1)
        d_gates = jnp.stack(
            [jnp.sum(jnp.where(hot[k], slot_dgate[:, None], 0.0), axis=0) for k in range(TOP)], axis=1
        )
        scaled = (back[:, :D].astype(jnp.float32) * slot_gate[:, None]).astype(low)
        joined = jnp.concatenate([scaled, back[:, D:]], axis=1)
        gathered = lax.dot_general(
            table, joined, (((0,), (0,)), ((), ())), preferred_element_type=jnp.float32
        )
        outputs.append((middle + gathered[:, :D]).astype(low))
        gate_pull = jax.vjp(partial(gate_values, route_picks=picks), logits)[1]
        d_logits = gate_pull(d_gates)[0].astype(low)
        router_grad = router_grad + mm(two_low.T, d_logits)
        d_two = gathered[:, D:] + mm(d_logits, w_router.T)
        d_norm, gain_part = jax.vjp(rms_norm, middle, gains[1])[1](d_two)
        gain_two = gain_two + gain_part
        d_mid = d_resid + d_norm
        d_branch = d_mid.astype(low)
        mids.append(d_mid)
        d_branches.append(d_branch)
        d_attns.append(mm(d_branch, w_out.T).astype(low))
    d_attn = jnp.stack(d_attns)
    d_branch = jnp.concatenate(d_branches)
    out_grad = mm(attn.reshape(B * T, D).T, d_branch)
    delta = jnp.sum(
        (attn.astype(jnp.float32) * d_attn.astype(jnp.float32)).reshape(B, T, HEADS, HEAD_DIM), axis=-1
    )
    delta = jnp.transpose(delta, (0, 2, 1)).reshape(B, HEADS // 2, 2, T)
    dq, dk, dv, diag = attn_backward(line, q, kv, d_attn, qf, kf, lse, delta, c0)
    table_grad = table_from_diagonals(diag)

    d_normed = (mm(dk.reshape(B * K, D), w_k.T) + mm(dv.reshape(B * K, D), w_v.T)).reshape(B, K, D)
    carried = d_normed[:, :T]
    for hop in range(hops - 1, -1, -1):
        start = (hops - hop) * T
        carried = (
            passed_along(carried.astype(low), "ctx", -1).astype(jnp.float32)
            + d_normed[:, start : start + T]
        )
    own = carried + mm(dq.reshape(B * T, D), w_q.T).reshape(B, T, D)
    normed_rows = normed.reshape(B * K, D)
    proj_grad = jnp.concatenate(
        [
            mm(normed_own.reshape(B * T, D).T, dq.reshape(B * T, D)),
            mm(normed_rows.T, dk.reshape(B * K, D)),
            mm(normed_rows.T, dv.reshape(B * K, D)),
        ],
        axis=1,
    ).astype(low)
    d_first, gain_one = jax.vjp(rms_norm, tokens.astype(jnp.float32), gains[0])[1](own)
    tokens_grad = (jnp.stack(mids) + d_first).astype(low)

    side = jnp.concatenate(
        [out_grad, jnp.pad(router_grad, ((0, 0), (0, 128 - experts)))], axis=1
    ).astype(low)
    side_part = lax.psum_scatter(side, ("dp", "ctx"), scatter_dimension=0, tiled=True)
    proj_part = lax.psum_scatter(proj_grad, ("dp", "ctx"), scatter_dimension=0, tiled=True)
    gains_total, table_total = lax.psum(
        (jnp.stack([gain_one, gain_two])[None], table_grad[None]), ("dp", "ctx")
    )
    wide = jnp.float32
    return (
        jnp.stack(outputs),
        tokens_grad,
        proj_part.astype(wide)[None],
        side_part[:, :D].astype(wide)[None],
        side_part[:, D : D + experts].astype(wide)[None],
        gains_total,
        table_total,
        up_grad.astype(wide)[None, None],
        dn_grad.astype(wide).T[None, None],
    )


def solution(mesh):
    in_specs = (
        P("dp", "ctx", None),
        P("dp", "ctx", None),
        P(None, ("dp", "ctx"), None),
        P(None, ("dp", "ctx"), None),
        P(None, ("dp", "ctx"), None),
        P(),
        P(),
        P(None, "dp", None, "ctx"),
        P(None, "dp", "ctx", None),
        P("dp", None),
        P("dp", "ctx", None),
    )
    out_specs = (
        P("dp", "ctx", None),
        P("dp", "ctx", None),
        P(None, ("dp", "ctx"), None),
        P(None, ("dp", "ctx"), None),
        P(None, ("dp", "ctx"), None),
        P(),
        P(),
        P(None, "dp", None, "ctx"),
        P(None, "dp", "ctx", None),
    )
    return jax.shard_map(
        on_device, mesh=mesh, in_specs=in_specs, out_specs=out_specs, check_vma=False
    )
```

```python
from functools import partial

import jax
import jax.numpy as jnp
from jax import lax
from jax.experimental import pallas as pl
from jax.experimental.pallas import tpu as pltpu
from jax.sharding import PartitionSpec as P


HEADS=12; HEAD_DIM=64; NB=32; WIN=1024; TOP=2
NEG=-1e30
BUCKET_EDGES = [16, 21, 27, 35, 45, 58, 76, 98, 128, 166, 215, 279, 362, 470, 609, 790]
QB=256; CB=256; SPAN=WIN+QB; GROWS=SPAN+128; GSEG=GROWS//128

NT=(((1,),(1,)),((),()))
NN=(((1,),(0,)),((),()))


def dot(a,b,dims): return lax.dot_general(a,b,dims,preferred_element_type=jnp.float32)


def bucket_index(distance):
    edge_values = jnp.array(BUCKET_EDGES, dtype=jnp.int32)
    passed = jnp.sum((distance[..., None] >= edge_values).astype(jnp.int32), axis=-1)
    return jnp.where(distance < 16, distance, 15 + passed)


def bias_line(table):
    n = GROWS + 128
    d = jnp.arange(n, dtype=jnp.int32) - 256
    hot = (jnp.clip(bucket_index(d),0,NB-1)[:,None]==jnp.arange(NB)).astype(jnp.float32)
    line = jnp.einsum("nb,bh->hn", hot, table, precision=lax.Precision.HIGHEST)
    line = jnp.where((d>=0)&(d<WIN), line, NEG)
    return line.reshape(HEADS//2,2,n)


def spread_bias(line_ref, g_ref):
    for hh in range(2):
        for a in range(GSEG):
            start = (GSEG-1-a)*128
            seg = line_ref[0, hh:hh+1, start:start+256]
            x = jnp.broadcast_to(seg,(128,256))
            x = pltpu.roll(x,0,1,stride=1,stride_axis=0)
            g_ref[hh, a*128:(a+1)*128,:] = x[:,128:256]


def bias_chunk(g_ref, hh, r):
    o = pl.multiple_of(r*CB,CB) if not isinstance(r,int) else r*CB
    return jnp.concatenate([g_ref[hh, pl.ds(o+128,CB),:], g_ref[hh, pl.ds(o,CB),:]],axis=1)


def rows8(x, op):
    return op(x.reshape(x.shape[0]//8,8,x.shape[1]),axis=0)


def fwd_kernel(c0, line_ref, q_ref, k_ref, v_ref, qf_ref, kf_ref, o_ref, lse_ref, g_ref, kh_ref, qh_ref, vt_ref, s_ref, ot_ref):
    T=q_ref.shape[1]

    @pl.when(pl.program_id(1)==0)
    def _(): spread_bias(line_ref,g_ref)

    lane = lax.broadcasted_iota(jnp.int32,(1,128),1)
    vt_ref[...] = v_ref[0].T
    for hh in range(2):
        mine = (lane//64)==hh
        kh_ref[...] = jnp.where(mine,k_ref[0],kf_ref[0])
        qh_ref[...] = jnp.where(mine,q_ref[0],qf_ref[0])
        for b in range(T//QB):
            qb = qh_ref[b*QB:(b+1)*QB,:]
            mx=None
            for r in range(SPAN//CB):
                base=b*QB+c0+r*CB
                s=dot(kh_ref[base:base+CB,:],qb,NT)+bias_chunk(g_ref,hh,r)
                s_ref[r]=s
                m8=rows8(s,jnp.max)
                mx=m8 if mx is None else jnp.maximum(mx,m8)
            m=jnp.max(mx,axis=0,keepdims=True)
            tot=None; acc=None
            for r in range(SPAN//CB):
                base=b*QB+c0+r*CB
                p=jnp.exp(s_ref[r]-m)
                t8=rows8(p,jnp.sum)
                tot=t8 if tot is None else tot+t8
                d=dot(vt_ref[64*hh:64*hh+64,base:base+CB],p.astype(jnp.bfloat16),NN)
                acc=d if acc is None else acc+d
            l=jnp.sum(tot,axis=0,keepdims=True)
            ot_ref[64*hh:64*hh+64,b*QB:(b+1)*QB]=acc*(1.0/l)
            lse_ref[0,0,hh:hh+1,b*QB:(b+1)*QB]=m+jnp.log(l)
    o_ref[0]=ot_ref[...].T.astype(jnp.bfloat16)


def attn_forward(line,q,kv,qf,kf,c0,m0,B):
    _,T,D=q.shape; K=kv.shape[1]; PR=D//128
    return pl.pallas_call(
        partial(fwd_kernel,c0),
        grid=(PR,B),
        in_specs=[pl.BlockSpec((1,2,line.shape[2]),lambda p,m:(p,0,0)),
                  pl.BlockSpec((1,T,128),lambda p,m:(m0+m,0,p)),
                  pl.BlockSpec((1,K,128),lambda p,m:(m0+m,0,p)),
                  pl.BlockSpec((1,K,128),lambda p,m:(m0+m,0,PR+p)),
                  pl.BlockSpec((1,T,128),lambda p,m:(m0+m,0,0)),
                  pl.BlockSpec((1,K,128),lambda p,m:(m0+m,0,0))],
        out_specs=[pl.BlockSpec((1,T,128),lambda p,m:(m,0,p)),
                   pl.BlockSpec((1,1,2,T),lambda p,m:(m,p,0,0))],
        out_shape=[jax.ShapeDtypeStruct((B,T,D),jnp.bfloat16),jax.ShapeDtypeStruct((B,PR,2,T),jnp.float32)],
        scratch_shapes=[pltpu.VMEM((2,GROWS,128),jnp.float32),pltpu.VMEM((K,128),jnp.bfloat16),pltpu.VMEM((T,128),jnp.bfloat16),
                        pltpu.VMEM((128,K),jnp.bfloat16),pltpu.VMEM((SPAN//CB,CB,QB),jnp.float32),pltpu.VMEM((128,T),jnp.float32)],
        cost_estimate=pl.CostEstimate(flops=4*B*D*T*SPAN,bytes_accessed=2*B*D*(2*T+2*K),transcendentals=B*HEADS*T*SPAN),
    )(line,q,kv,kv,qf,kf)


def bwd_kernel(c0, line_ref, q_ref, k_ref, v_ref, g_ref_in, qf_ref, kf_ref, lse_ref, dl_ref, dq_ref, dk_ref, dv_ref, tg_ref,
               g_ref, kh_ref, qh_ref, qz_ref, dz_ref, kt_ref, dk_acc, dv_acc, dqt_acc, t_acc):
    T=q_ref.shape[1]
    last=pl.num_programs(1)-1

    @pl.when(pl.program_id(1)==0)
    def _():
        spread_bias(line_ref,g_ref)
        t_acc[...]=jnp.zeros_like(t_acc)

    lane = lax.broadcasted_iota(jnp.int32,(1,128),1)
    kt_ref[...] = k_ref[0].T
    dk_acc[...]=jnp.zeros_like(dk_acc)
    dv_acc[...]=jnp.zeros_like(dv_acc)
    for hh in range(2):
        mine = (lane//64)==hh
        kh_ref[hh] = jnp.where(mine,k_ref[0],kf_ref[0])
        qh_ref[hh] = jnp.where(mine,q_ref[0],qf_ref[0])
        qz_ref[hh] = jnp.where(mine,q_ref[0],jnp.zeros_like(q_ref[0]))
        dz_ref[hh] = jnp.where(mine,g_ref_in[0],jnp.zeros_like(q_ref[0]))
    dqt_acc[...]=jnp.zeros_like(dqt_acc)
    nb=T//QB

    def step(r,carry):
        for b in range(nb):
            for hh in range(2):
                base=pl.multiple_of(b*QB+c0+r*CB,128)
                keys=pl.ds(base,CB)
                rows=slice(b*QB,(b+1)*QB)
                s=dot(kh_ref[hh,keys,:],qh_ref[hh,rows,:],NT)+bias_chunk(g_ref,hh,r)
                p=jnp.exp(s-lse_ref[0,0,hh:hh+1,rows])
                dp=dot(v_ref[0,keys,:],dz_ref[hh,rows,:],NT)
                ds=p*(dp-dl_ref[0,0,hh:hh+1,rows])
                dsb=ds.astype(jnp.bfloat16)
                dv_acc[keys,:]+=dot(p.astype(jnp.bfloat16),dz_ref[hh,rows,:],NN)
                dk_acc[keys,:]+=dot(dsb,qz_ref[hh,rows,:],NN)
                dqt_acc[64*hh:64*hh+64,rows]+=dot(kt_ref[64*hh:64*hh+64,keys],dsb,NN)
                o=pl.multiple_of(r*CB,CB)
                t_acc[hh,pl.ds(o+128,CB),:]+=ds[:,:128]
                t_acc[hh,pl.ds(o,CB),:]+=ds[:,128:]
        return carry

    lax.fori_loop(0,SPAN//CB,step,0)
    dk_ref[0]=dk_acc[...].astype(jnp.bfloat16)
    dv_ref[0]=dv_acc[...].astype(jnp.bfloat16)
    dq_ref[0]=(dqt_acc[...].T*(HEAD_DIM**-0.5)).astype(jnp.bfloat16)

    @pl.when(pl.program_id(1)==last)
    def _():
        flip=(lax.broadcasted_iota(jnp.int32,(128,128),0)+lax.broadcasted_iota(jnp.int32,(128,128),1)==127).astype(jnp.float32)
        for hh in range(2):
            for a in range(GSEG):
                blk=lax.dot_general(flip,t_acc[hh,a*128:(a+1)*128,:],NN,precision=lax.Precision.HIGHEST,preferred_element_type=jnp.float32)
                x=jnp.concatenate([blk,jnp.zeros_like(blk)],axis=1)
                x=pltpu.roll(x,0,1,stride=1,stride_axis=0)
                tg_ref[0,hh,a:a+1,:]=jnp.sum(x,axis=0,keepdims=True)


def attn_backward(line,q,kv,do,qf,kf,lse,dl,c0,m0):
    T,D=q.shape[1:]; B=do.shape[0]; K=kv.shape[1]; PR=D//128
    return pl.pallas_call(
        partial(bwd_kernel,c0),
        grid=(PR,B),
        in_specs=[pl.BlockSpec((1,2,line.shape[2]),lambda p,m:(p,0,0)),
                  pl.BlockSpec((1,T,128),lambda p,m:(m0+m,0,p)),
                  pl.BlockSpec((1,K,128),lambda p,m:(m0+m,0,p)),
                  pl.BlockSpec((1,K,128),lambda p,m:(m0+m,0,PR+p)),
                  pl.BlockSpec((1,T,128),lambda p,m:(m,0,p)),
                  pl.BlockSpec((1,T,128),lambda p,m:(m0+m,0,0)),
                  pl.BlockSpec((1,K,128),lambda p,m:(m0+m,0,0)),
                  pl.BlockSpec((1,1,2,T),lambda p,m:(m,p,0,0)),
                  pl.BlockSpec((1,1,2,T),lambda p,m:(m,p,0,0))],
        out_specs=[pl.BlockSpec((1,T,128),lambda p,m:(m,0,p)),
                   pl.BlockSpec((1,K,128),lambda p,m:(m,0,p)),
                   pl.BlockSpec((1,K,128),lambda p,m:(m,0,p)),
                   pl.BlockSpec((1,2,GSEG,256),lambda p,m:(p,0,0,0))],
        out_shape=[jax.ShapeDtypeStruct((B,T,D),jnp.bfloat16),jax.ShapeDtypeStruct((B,K,D),jnp.bfloat16),
                   jax.ShapeDtypeStruct((B,K,D),jnp.bfloat16),jax.ShapeDtypeStruct((PR,2,GSEG,256),jnp.float32)],
        scratch_shapes=[pltpu.VMEM((2,GROWS,128),jnp.float32),pltpu.VMEM((2,K,128),jnp.bfloat16),pltpu.VMEM((2,T,128),jnp.bfloat16),
                        pltpu.VMEM((2,T,128),jnp.bfloat16),pltpu.VMEM((2,T,128),jnp.bfloat16),pltpu.VMEM((128,K),jnp.bfloat16),
                        pltpu.VMEM((K,128),jnp.float32),pltpu.VMEM((K,128),jnp.float32),pltpu.VMEM((128,T),jnp.float32),
                        pltpu.VMEM((2,GROWS,128),jnp.float32)],
        cost_estimate=pl.CostEstimate(flops=10*B*D*T*SPAN,bytes_accessed=2*B*D*(2*T+2*K)*2,transcendentals=B*HEADS*T*SPAN),
    )(line,q,kv,kv,do,qf,kf,lse,dl)


def table_from_diagonals(diag):
    d = WIN+128-128*jnp.arange(GSEG)[:,None]+(jnp.arange(256)[None,:]-127)
    hot=(jnp.clip(bucket_index(d),0,NB-1)[...,None]==jnp.arange(NB)).astype(jnp.float32)
    hot=hot*((d>=0)&(d<WIN)).astype(jnp.float32)[...,None]
    h=diag.reshape(HEADS,GSEG*256)
    return jnp.einsum("hn,nb->bh",h,hot.reshape(GSEG*256,NB),precision=lax.Precision.HIGHEST)


def features(qdoc,kdoc,kvalid):
    lane=jnp.arange(128)%64
    qf=(qdoc[...,None]==lane).astype(jnp.bfloat16)
    bad=(kdoc[...,None]!=lane)|~kvalid[...,None]
    kf=jnp.where(bad&(lane<8),NEG,0.0).astype(jnp.bfloat16)
    return qf,kf


GELU_C = 0.7978845608028654
GELU_A = 0.044715


def row_step(rows):
    for size in (256, 128, 64, 32, 16):
        if rows % size == 0:
            return size
    return rows


def expert_kernel(with_prior, xg_ref, up_ref, dn_ref, *refs):
    if with_prior:
        pu_ref, pd_ref, ret_ref, ug_ref, dg_ref, acc, xt, gt, hb, zb = refs
    else:
        ret_ref, ug_ref, dg_ref, acc, xt, gt, hb, zb = refs
    R = xg_ref.shape[0]
    D = xg_ref.shape[1] // 2
    RB = row_step(R)

    @pl.when(pl.program_id(0) == 0)
    def _():
        xt[...] = xg_ref[:, :D].T
        gt[...] = xg_ref[:, D:].T
        acc[...] = jnp.zeros_like(acc)

    up = up_ref[...]
    dn = dn_ref[...]

    def block(i, carry):
        rs = pl.ds(pl.multiple_of(i * RB, RB), RB)
        z = dot(xg_ref[rs, :D], up, NN)
        dh = dot(xg_ref[rs, D:], dn, NT)
        zz = z * z
        t = jnp.tanh(z * (GELU_C + (GELU_C * GELU_A) * zz))
        half = 0.5 + 0.5 * t
        h = (z * half).astype(jnp.bfloat16)
        slope = half + z * (0.5 - 0.5 * t * t) * (GELU_C + (3.0 * GELU_C * GELU_A) * zz)
        dz = (dh * slope).astype(jnp.bfloat16)
        hb[rs, :] = h
        zb[rs, :] = dz
        acc[rs, :D] += dot(h, dn, NN)
        acc[rs, D:] += dot(dz, up, NT)
        return carry

    lax.fori_loop(0, R // RB, block, 0)
    ug = dot(xt[...], zb[...], NN)
    dg = dot(gt[...], hb[...], NN)
    if with_prior:
        ug += pu_ref[...]
        dg += pd_ref[...]
    ug_ref[...] = ug.astype(ug_ref.dtype)
    dg_ref[...] = dg.astype(dg_ref.dtype)

    @pl.when(pl.program_id(0) == pl.num_programs(0) - 1)
    def _():
        ret_ref[...] = acc[...].astype(jnp.bfloat16)


def expert_step(xg, up, dn, prior, last):
    R, D2 = xg.shape
    D, F = up.shape
    FC = 512
    wide = pl.BlockSpec((D, FC), lambda f: (0, f))
    tall = pl.BlockSpec((FC, D), lambda f: (f, 0))
    whole = pl.BlockSpec((R, D2), lambda f: (0, 0))
    grad_type = jnp.bfloat16 if last else jnp.float32
    return pl.pallas_call(
        partial(expert_kernel, prior is not None),
        grid=(F // FC,),
        in_specs=[whole, wide, tall] + ([wide, wide] if prior is not None else []),
        out_specs=[whole, wide, wide],
        out_shape=[
            jax.ShapeDtypeStruct((R, D2), jnp.bfloat16),
            jax.ShapeDtypeStruct((D, F), grad_type),
            jax.ShapeDtypeStruct((D, F), grad_type),
        ],
        scratch_shapes=[
            pltpu.VMEM((R, D2), jnp.float32),
            pltpu.VMEM((D, R), jnp.bfloat16),
            pltpu.VMEM((D, R), jnp.bfloat16),
            pltpu.VMEM((R, FC), jnp.bfloat16),
            pltpu.VMEM((R, FC), jnp.bfloat16),
        ],
        cost_estimate=pl.CostEstimate(
            flops=12 * R * D * F, bytes_accessed=8 * D * F + 8 * R * D, transcendentals=R * F
        ),
    )(xg, up, dn, *(prior if prior is not None else ()))


MESH = pl.DeviceIdType.MESH


def partners():
    d, z = lax.axis_index("dp"), lax.axis_index("ctx")
    core, x, y = d % 2, (d // 2) % 2, d // 4
    return d, z, core, x, y, d + 1 - 2 * core, d + 2 - 4 * x, d + 4 - 8 * y


def greet(peers):
    barrier = pltpu.get_barrier_semaphore()
    for peer in peers:
        pl.semaphore_signal(barrier, inc=1, device_id=peer, device_id_type=MESH)
    pl.semaphore_wait(barrier, len(peers))


def sum_kernel(widths, split, Z, *refs):
    n = len(widths)
    parts, small, outs, small_out = refs[:n], refs[n], refs[n + 1 : 2 * n + 1], refs[2 * n + 1]
    got1 = refs[2 * n + 2 : 3 * n + 2]
    keep1 = refs[3 * n + 2 : 4 * n + 2]
    got2 = refs[4 * n + 2 : 5 * n + 2]
    keep2 = refs[5 * n + 2 : 6 * n + 2]
    got3 = refs[6 * n + 2 : 7 * n + 2]
    keep3 = refs[7 * n + 2 : 8 * n + 2]
    got4 = refs[8 * n + 2 : 9 * n + 2]
    s_keep, s_got, send, recv = refs[9 * n + 2 :]
    d, z, core, x, y, pc, px, py = partners()
    zs = [(z + k) % Z for k in range(1, Z)]
    peers = [(pc, z), (px, z), (py, z)] + [(d, t) for t in zs]
    greet(peers)
    low, wide = jnp.bfloat16, jnp.float32

    def push(src, dst, i, peer):
        copy = pltpu.make_async_remote_copy(
            src_ref=src,
            dst_ref=dst,
            send_sem=send.at[i],
            recv_sem=recv.at[i],
            device_id=peer,
            device_id_type=MESH,
        )
        copy.start()
        return copy

    s_keep[0] = small[...]

    stage = [push(parts[j].at[:, :, 1 - core], got1[j], j, (pc, z)) for j in range(n)]
    tiny = push(s_keep.at[0], s_got.at[0], 4 * n, (pc, z))
    order = list(range(n))
    stage2 = [None] * n
    for j in order:
        stage[j].wait()
        first = j < split
        for a in range(2):
            for b in range(2):
                if first:
                    keep1[j][b, a] = (parts[j][a, b, core].astype(wide) + got1[j][a, b].astype(wide)).astype(low)
                else:
                    keep1[j][a, b] = (parts[j][a, b, core].astype(wide) + got1[j][a, b].astype(wide)).astype(low)
        mine, peer = (x, (px, z)) if first else (y, (py, z))
        stage2[j] = push(keep1[j].at[1 - mine], got2[j], n + j, peer)
    tiny.wait()
    s_keep[1] = s_keep[0] + s_got[0]
    tiny = push(s_keep.at[1], s_got.at[1], 4 * n + 1, (px, z))
    stage3 = [None] * n
    for j in order:
        stage2[j].wait()
        first = j < split
        mine, then, peer = (x, y, (py, z)) if first else (y, x, (px, z))
        for a in range(2):
            keep2[j][a] = (keep1[j][mine, a].astype(wide) + got2[j][a].astype(wide)).astype(low)
        stage3[j] = push(keep2[j].at[1 - then], got3[j], 2 * n + j, peer)
    tiny.wait()
    s_keep[2] = s_keep[1] + s_got[1]
    tiny = push(s_keep.at[2], s_got.at[2], 4 * n + 2, (py, z))
    stage4 = []
    base = 4 * n + 3
    for j in order:
        stage3[j].wait()
        then = y if j < split else x
        keep3[j][...] = (keep2[j][then].astype(wide) + got3[j][...].astype(wide)).astype(low)
        for k in range(Z - 1):
            stage4.append(push(keep3[j].at[zs[k]], got4[j].at[k], base + j * (Z - 1) + k, (d, zs[k])))
    tiny.wait()
    s_keep[3] = s_keep[2] + s_got[2]
    base = base + n * (Z - 1)
    tinies = [push(s_keep.at[3], s_got.at[3 + z], base + k, (d, zs[k])) for k in range(Z - 1)]
    for copy in stage4:
        copy.wait()
    for j in order:
        total = keep3[j][z].astype(wide)
        for k in range(Z - 1):
            total = total + got4[j][k].astype(wide)
        outs[j][...] = total
    for copy in tinies:
        copy.wait()
    total = None
    for t in range(Z):
        term = jnp.where(z == t, s_keep[3], s_got[3 + t])
        total = term if total is None else total + term
    small_out[...] = total


def sum_over_all(parts, split, small):
    Z = lax.axis_size("ctx")
    rows = parts[0].shape[0] // (8 * Z)
    widths = [p.shape[1] for p in parts]
    n = len(parts)
    views = [p.astype(jnp.bfloat16).reshape(2, 2, 2, Z, rows, w) for p, w in zip(parts, widths)]
    vm = pl.BlockSpec(memory_space=pltpu.VMEM)
    low = jnp.bfloat16

    def buf(*lead):
        return [pltpu.VMEM(lead + (rows, w), low) for w in widths]

    sems = 4 * n + 3 + n * (Z - 1) + (Z - 1)
    out = pl.pallas_call(
        partial(sum_kernel, widths, split, Z),
        in_specs=[vm] * (n + 1),
        out_specs=[vm] * (n + 1),
        out_shape=[jax.ShapeDtypeStruct((rows, w), jnp.float32) for w in widths]
        + [jax.ShapeDtypeStruct(small.shape, jnp.float32)],
        scratch_shapes=buf(2, 2, Z) + buf(2, 2, Z) + buf(2, Z) + buf(2, Z) + buf(Z) + buf(Z) + buf(Z - 1)
        + [
            pltpu.VMEM((4,) + small.shape, jnp.float32),
            pltpu.VMEM((3 + Z,) + small.shape, jnp.float32),
            pltpu.SemaphoreType.DMA((sems,)),
            pltpu.SemaphoreType.DMA((sems,)),
        ],
        compiler_params=pltpu.CompilerParams(collective_id=1, has_side_effects=True),
    )(*views, small)
    return out[:n], out[n]


EPS = 1e-06


def passed_along(block, axis, distance):
    devices = range(lax.axis_size(axis))
    route = [(i - distance, i) for i in devices if i - distance in devices]
    return lax.ppermute(block, axis, route)


def rms_norm(operand, gain_vec):
    return operand * lax.rsqrt(jnp.mean(operand * operand, axis=-1, keepdims=True) + EPS) * gain_vec


def doc_of(positions, lengths):
    bounds = jnp.cumsum(lengths)[:-1]
    return jnp.sum((positions[:, None] >= bounds[None, :]).astype(jnp.int32), axis=-1)


def gate_values(logits, route_picks):
    soft_probs = jax.nn.softmax(logits, axis=-1)
    chosen = jnp.sum(soft_probs[:, None, :] * route_picks, axis=-1)
    return chosen / jnp.sum(chosen, axis=-1, keepdims=True)


def exchange(payload, ranks):
    shape = payload.shape
    blocks = payload.reshape(ranks, shape[0] // ranks, shape[1])
    return lax.all_to_all(blocks, "dp", split_axis=0, concat_axis=0, tiled=True).reshape(shape)


def mm(a, b):
    return jnp.dot(a, b, preferred_element_type=jnp.float32)


def layer(
    tokens,
    cotangent,
    proj_weights,
    out_weights,
    router_weights,
    norm_gains,
    bias_table,
    up_weights,
    down_weights,
    doc_lengths,
    routes,
):
    B, T, D = tokens.shape
    low = jnp.bfloat16
    ranks = lax.axis_size("dp")
    experts = ranks * up_weights.shape[1]
    capacity = max(2, 5 * TOP * T // (4 * experts))
    slots = experts * capacity
    hops = (WIN + T - 2) // T
    K = (hops + 1) * T
    c0 = K - T - WIN
    base_pos = lax.axis_index("ctx") * T

    x_own = tokens
    pieces = [x_own]
    moving = x_own
    for _ in range(hops):
        moving = passed_along(moving, "ctx", 1)
        pieces.append(moving)
    x_all = jnp.concatenate(pieces[::-1], axis=1)

    router_pad = jnp.pad(router_weights[0], ((0, 0), (0, 128 - experts)))
    dense = jnp.concatenate([proj_weights[0], out_weights[0], router_pad], axis=1).astype(low)
    dense_full = lax.all_gather(dense, ("dp", "ctx"), axis=0, tiled=True)
    up_full = lax.all_gather(up_weights[0, 0].astype(low), "ctx", axis=1, tiled=True)
    dn_full = lax.all_gather(down_weights[0, 0].astype(low), "ctx", axis=0, tiled=True)
    w_q, w_k, w_v = (dense_full[:, i * D : (i + 1) * D] for i in range(3))
    w_kv = dense_full[:, D : 3 * D]
    w_out = dense_full[:, 3 * D : 4 * D]
    w_router = dense_full[:, 4 * D : 4 * D + experts]
    gains = norm_gains[0]

    line = bias_line(bias_table[0])
    rows = jnp.arange(T, dtype=jnp.int32)
    key_pos = base_pos - (K - T) + jnp.arange(K, dtype=jnp.int32)
    key_doc = jnp.stack([doc_of(key_pos, doc_lengths[m]) for m in range(B)])
    key_ok = jnp.broadcast_to(key_pos >= 0, (B, K))
    qf, kf = features(key_doc[:, K - T :], key_doc, key_ok)

    normed = rms_norm(x_all.astype(jnp.float32), gains[0]).astype(low)
    kv = mm(normed.reshape(B * K, D), w_kv).astype(low).reshape(B, K, 2 * D)
    normed_own = normed[:, K - T :]
    q = (mm(normed_own.reshape(B * T, D), w_q).astype(low) * low(HEAD_DIM**-0.5)).reshape(B, T, D)

    expert_ids = jnp.arange(experts, dtype=jnp.int32)
    slot_range = jnp.arange(slots, dtype=jnp.int32)
    kept = []
    attns = []
    lses = []
    for m in range(B):
        attn, lse = attn_forward(line, q, kv, qf, kf, c0, m, 1)
        attn = attn[0]
        if kept:
            attn, _ = lax.optimization_barrier((attn, kept[-1][-2]))
        attns.append(attn)
        lses.append(lse)
        route_now = routes[m]
        picks = (route_now[:, :, None] == expert_ids).astype(jnp.float32)
        order_hot = (jnp.transpose(route_now).reshape(-1)[:, None] == expert_ids[None, :]).astype(
            jnp.int32
        )
        running = jnp.cumsum(order_hot, axis=0)
        slot_pos = (jnp.sum(running * order_hot, axis=-1) - 1).reshape(TOP, T)
        slot_ids = jnp.transpose(route_now) * capacity + slot_pos
        slot_ids = jnp.where(slot_pos < capacity, slot_ids, slots)
        hot = slot_ids[:, None, :] == slot_range[None, :, None]
        table = (hot[0] | hot[1]).astype(low)

        resid = tokens[m].astype(jnp.float32)
        d_out = cotangent[m]
        middle = resid + mm(attns[m], w_out)
        two_low = rms_norm(middle, gains[1]).astype(low)
        logits = mm(two_low, w_router)
        gates = gate_values(logits, picks)
        slot_gate = jnp.sum(
            jnp.where(hot[0], gates[None, :, 0], 0.0) + jnp.where(hot[1], gates[None, :, 1], 0.0),
            axis=1,
        )
        sent = mm(table, jnp.concatenate([two_low, d_out], axis=1))
        d_rows = sent[:, D:].astype(low)
        payload = jnp.concatenate(
            [sent[:, :D].astype(low), (sent[:, D:] * slot_gate[:, None]).astype(low)], axis=1
        )
        received = exchange(payload, ranks)
        kept.append((picks, hot, table, middle, two_low, logits, slot_gate, d_rows, payload, received))

    prior = None
    returned = []
    for m in range(B):
        last = m == B - 1
        received = kept[m][-1]
        back, up_part, dn_part = expert_step(received, up_full, dn_full, prior, last)
        prior = (up_part, dn_part)
        if not last:
            back, ahead = lax.optimization_barrier((back, kept[m + 1][-1]))
            kept[m + 1] = kept[m + 1][:-1] + (ahead,)
        returned.append(exchange(back, ranks))
    up_part, dn_part = prior
    up_grad = lax.psum_scatter(up_part, "ctx", scatter_dimension=1, tiled=True)
    dn_grad = lax.psum_scatter(dn_part, "ctx", scatter_dimension=1, tiled=True)

    outputs = []
    router_grad = 0.0
    out_grad = 0.0
    gain_one = 0.0
    gain_two = 0.0
    table_grad = 0.0
    tokens_grads = []
    q_grad = k_grad = v_grad = 0.0
    chains = []
    for m in range(B):
        picks, hot, table, middle, two_low, logits, slot_gate, d_rows, _, _ = kept[m]
        back = returned[m]
        if chains:
            back, _ = lax.optimization_barrier((back, delta))
        d_resid = cotangent[m].astype(jnp.float32)
        slot_dgate = jnp.sum(d_rows.astype(jnp.float32) * back[:, :D].astype(jnp.float32), axis=1)
        d_gates = jnp.stack(
            [jnp.sum(jnp.where(hot[k], slot_dgate[:, None], 0.0), axis=0) for k in range(TOP)], axis=1
        )
        scaled = (back[:, :D].astype(jnp.float32) * slot_gate[:, None]).astype(low)
        joined = jnp.concatenate([scaled, back[:, D:]], axis=1)
        gathered = lax.dot_general(
            table, joined, (((0,), (0,)), ((), ())), preferred_element_type=jnp.float32
        )
        outputs.append((middle + gathered[:, :D]).astype(low))
        gate_pull = jax.vjp(partial(gate_values, route_picks=picks), logits)[1]
        d_logits = gate_pull(d_gates)[0].astype(low)
        router_grad = router_grad + mm(two_low.T, d_logits)
        d_two = gathered[:, D:] + mm(d_logits, w_router.T)
        d_norm, gain_part = jax.vjp(rms_norm, middle, gains[1])[1](d_two)
        gain_two = gain_two + gain_part
        d_mid = d_resid + d_norm
        d_branch = d_mid.astype(low)
        d_attn = mm(d_branch, w_out.T).astype(low)
        out_grad = out_grad + mm(attns[m].T, d_branch)
        delta = jnp.sum(
            (attns[m].astype(jnp.float32) * d_attn.astype(jnp.float32)).reshape(T, HEADS, HEAD_DIM),
            axis=-1,
        )
        delta = delta.T.reshape(1, HEADS // 2, 2, T)
        dq, dk, dv, diag = attn_backward(
            line, q, kv, d_attn[None], qf, kf, lses[m], delta, c0, m
        )
        dq, dk, dv = dq[0], dk[0], dv[0]
        table_grad = table_grad + table_from_diagonals(diag)
        far = K - T
        d_far = mm(dk[:far], w_k.T) + mm(dv[:far], w_v.T)
        carried = d_far[:T]
        for hop in range(hops - 1, 0, -1):
            start = (hops - hop) * T
            carried = passed_along(carried.astype(low), "ctx", -1)
            carried = carried.astype(jnp.float32) + d_far[start : start + T]
        carried = passed_along(carried.astype(low), "ctx", -1)
        own = mm(dk[far:], w_k.T) + mm(dv[far:], w_v.T) + mm(dq, w_q.T)
        chains.append((carried, own, d_mid))
        q_grad = q_grad + mm(normed[m, far:].T, dq)
        k_grad = k_grad + mm(normed[m].T, dk)
        v_grad = v_grad + mm(normed[m].T, dv)
    for m in range(B):
        carried, own, d_mid = chains[m]
        d_first, gain_part = jax.vjp(rms_norm, tokens[m].astype(jnp.float32), gains[0])[1](
            own + carried.astype(jnp.float32)
        )
        gain_one = gain_one + gain_part
        tokens_grads.append((d_mid + d_first).astype(low))

    router_wide = jnp.pad(router_grad, ((0, 0), (0, 128 - experts)))
    small = jnp.concatenate([gain_one, gain_two, table_grad.reshape(-1)])
    if ranks == 8 and D % (16 * lax.axis_size("ctx")) == 0:
        small = jnp.pad(small, (0, 2048 - small.shape[0])).reshape(8, 256)
        parts, small = sum_over_all([q_grad, k_grad, router_wide, v_grad, out_grad], 3, small)
        small = small.reshape(-1)
        proj_part = jnp.concatenate([parts[0], parts[1], parts[3]], axis=1)
        router_part, out_part = parts[2], parts[4]
    else:
        joined = jnp.concatenate([q_grad, k_grad, v_grad, out_grad, router_wide], axis=1).astype(low)
        joined = lax.psum_scatter(joined, ("dp", "ctx"), scatter_dimension=0, tiled=True)
        joined = joined.astype(jnp.float32)
        small = lax.psum(small, ("dp", "ctx"))
        proj_part, out_part, router_part = (
            joined[:, : 3 * D],
            joined[:, 3 * D : 4 * D],
            joined[:, 4 * D :],
        )
    wide = jnp.float32
    return (
        jnp.stack(outputs),
        jnp.stack(tokens_grads),
        proj_part[None],
        out_part[None],
        router_part[None, :, :experts],
        small[: 2 * D].reshape(1, 2, D),
        small[2 * D : 2 * D + NB * HEADS].reshape(1, NB, HEADS),
        up_grad.astype(wide)[None, None],
        dn_grad.astype(wide).T[None, None],
    )


def solution(mesh):
    in_specs = (
        P("dp", "ctx", None),
        P("dp", "ctx", None),
        P(None, ("dp", "ctx"), None),
        P(None, ("dp", "ctx"), None),
        P(None, ("dp", "ctx"), None),
        P(),
        P(),
        P(None, "dp", None, "ctx"),
        P(None, "dp", "ctx", None),
        P("dp", None),
        P("dp", "ctx", None),
    )
    out_specs = (
        P("dp", "ctx", None),
        P("dp", "ctx", None),
        P(None, ("dp", "ctx"), None),
        P(None, ("dp", "ctx"), None),
        P(None, ("dp", "ctx"), None),
        P(),
        P(),
        P(None, "dp", None, "ctx"),
        P(None, "dp", "ctx", None),
    )
    return jax.shard_map(layer, mesh=mesh, in_specs=in_specs, out_specs=out_specs, check_vma=False)
```
